16 devices in a mesh: data: 16 (over z, y, x, core).
Axes of the slice: x: 2, y: 2, z: 2, core: 2. Of those that a mesh axis runs over, the one named last changes fastest.
Arguments:
- tokens: bfloat16 [16384, 1536], P('data')
- targets: bfloat16 [16384, 1536], P('data')
- w_in: bfloat16 [2, 1536, 8960], replicated
- w_out: bfloat16 [2, 8960, 1536], replicated
Outputs:
- output 1: float32 [2, 1536, 8960], P(None, 'data')
- output 2: float32 [2, 8960, 1536], P(None, 'data')
All inputs are finite; a program needn't handle non-finite values.
Results may differ from the reference program's by a relative error of at most 0.00605358.
Values are sent between devices in bfloat16 or wider.
A program may use at most 1 GiB of HBM per device.

```python
import jax
import jax.numpy as jnp
from jax import lax

D = 1536
FF = 8960
LAYERS = 2
TOKENS_DEV = 1024
DATA = 16
TOKENS = TOKENS_DEV * DATA


def setup_inputs(seed: int = 0) -> dict:
    key_root = jax.random.key(seed)
    key_tok, key_tgt, key_in, key_out = jax.random.split(key_root, 4)
    tokens = jax.random.normal(key_tok, (TOKENS, D), jnp.float32).astype(jnp.bfloat16)
    targets = (2.0 * jax.random.normal(key_tgt, (TOKENS, D), jnp.float32)).astype(jnp.bfloat16)
    w_in = (jax.random.normal(key_in, (LAYERS, D, FF), jnp.float32) * (D ** -0.5)).astype(jnp.bfloat16)
    w_out = (jax.random.normal(key_out, (LAYERS, FF, D), jnp.float32) * (0.5 * FF ** -0.5)).astype(jnp.bfloat16)
    return {"tokens": tokens, "targets": targets, "w_in": w_in, "w_out": w_out}


def gelu_act(pre_f32):
    return jax.nn.gelu(pre_f32, approximate=True)


def layer_forward(hidden, weights):
    w_first, w_second = weights
    pre_act = jnp.dot(hidden, w_first, preferred_element_type=jnp.float32).astype(jnp.bfloat16)
    act_out = gelu_act(pre_act.astype(jnp.float32)).astype(jnp.bfloat16)
    branch = jnp.dot(act_out, w_second, preferred_element_type=jnp.float32)
    new_hidden = (hidden.astype(jnp.float32) + branch).astype(jnp.bfloat16)
    return new_hidden, (hidden, pre_act, act_out)


def layer_backward(grad_h, saved_items):
    hidden, pre_act, act_out, w_first, w_second = saved_items
    grad_second = jnp.dot(act_out.T, grad_h, preferred_element_type=jnp.float32)
    grad_act = jnp.dot(grad_h, w_second.T, preferred_element_type=jnp.float32).astype(jnp.bfloat16)
    _, pullback = jax.vjp(gelu_act, pre_act.astype(jnp.float32))
    grad_pre = pullback(grad_act.astype(jnp.float32))[0].astype(jnp.bfloat16)
    grad_first = jnp.dot(hidden.T, grad_pre, preferred_element_type=jnp.float32)
    grad_below = jnp.dot(grad_pre, w_first.T, preferred_element_type=jnp.float32)
    new_grad = (grad_h.astype(jnp.float32) + grad_below).astype(jnp.bfloat16)
    return new_grad, (grad_first, grad_second)


def block_grads(tok_rows, tgt_rows, w_in, w_out):
    top_hidden, saved_fwd = lax.scan(layer_forward, tok_rows, (w_in, w_out))
    grad_top = ((top_hidden.astype(jnp.float32) - tgt_rows.astype(jnp.float32)) * (TOKENS ** -0.5)).astype(jnp.bfloat16)
    _, layer_grads = lax.scan(layer_backward, grad_top, (saved_fwd[0], saved_fwd[1], saved_fwd[2], w_in, w_out), reverse=True)
    return layer_grads


def reference(tokens, targets, w_in, w_out):
    tok_blocks = tokens.reshape(DATA, TOKENS_DEV, D)
    tgt_blocks = targets.reshape(DATA, TOKENS_DEV, D)

    def accumulate(carry, row_pair):
        grad_first, grad_second = block_grads(row_pair[0], row_pair[1], w_in, w_out)
        return (carry[0] + grad_first, carry[1] + grad_second), None

    zero_sums = (jnp.zeros((LAYERS, D, FF), jnp.float32), jnp.zeros((LAYERS, FF, D), jnp.float32))
    (sum_first, sum_second), _ = lax.scan(accumulate, zero_sums, (tok_blocks, tgt_blocks))
    return sum_first, sum_second
```

```python
import functools

import jax
import jax.numpy as jnp
from jax import lax
from jax.experimental import pallas as pl
from jax.experimental.pallas import tpu as pltpu
from jax.sharding import PartitionSpec as P


AXIS = "data"
DEVICES = 16
CORE, X, Y, Z = 1, 2, 4, 8
GELU_S = 0.7978845608028654
GELU_C = 0.044715


def groups_of(bits):
    spans = []
    for base in range(DEVICES):
        if base & bits == 0:
            spans.append([base | sub for sub in range(DEVICES) if sub & ~bits == 0])
    return spans


def swap(value, bits):
    return lax.ppermute(value, AXIS, [(i, i ^ bits) for i in range(DEVICES)])


def gelu_parts(u):
    sq = u * u
    th = jnp.tanh(u * (GELU_S + (GELU_S * GELU_C) * sq))
    cdf = 0.5 + 0.5 * th
    slope = cdf + (0.5 * u) * (1.0 - th * th) * (GELU_S + (3.0 * GELU_S * GELU_C) * sq)
    return u * cdf, slope


def rounded(value):
    return value.astype(jnp.bfloat16).astype(jnp.float32)


def dot_nn(a, b):
    return jnp.dot(a, b, preferred_element_type=jnp.float32)


def dot_nt(a, b):
    return lax.dot_general(a, b, (((1,), (1,)), ((), ())), preferred_element_type=jnp.float32)


def forward_body(scale, parts, *refs):
    if scale is None:
        hidden, w_in, w_out, out, acc = refs
    else:
        hidden, w_in, w_out, target, pre_out, out, acc = refs
    step = pl.program_id(0)
    rows = hidden.shape[0] // parts

    @pl.when(step == 0)
    def _():
        acc[...] = hidden[...].astype(jnp.float32)

    for part in range(parts):
        at = pl.ds(part * rows, rows)
        pre = dot_nn(hidden[at], w_in[0]).astype(jnp.bfloat16)
        if scale is not None:
            pre_out[at] = pre
        act = gelu_parts(pre.astype(jnp.float32))[0].astype(jnp.bfloat16)
        acc[at] += dot_nn(act, w_out[0])

    @pl.when(step == pl.num_programs(0) - 1)
    def _():
        if scale is None:
            out[...] = acc[...].astype(jnp.bfloat16)
        else:
            out[...] = ((rounded(acc[...]) - target[...].astype(jnp.float32)) * scale).astype(jnp.bfloat16)


FF_TILE = 1280


def layer_specs(layer, rows, width):
    whole = pl.BlockSpec((rows, width), lambda j: (0, 0))
    w_in = pl.BlockSpec((1, width, FF_TILE), lambda j: (layer, 0, j))
    w_out = pl.BlockSpec((1, FF_TILE, width), lambda j: (layer, j, 0))
    pre = pl.BlockSpec((rows, FF_TILE), lambda j: (0, j))
    return whole, w_in, w_out, pre


def layer_params(rows, width, ff):
    return dict(
        compiler_params=pltpu.CompilerParams(vmem_limit_bytes=62 * 2**20, dimension_semantics=("arbitrary",)),
        cost_estimate=pl.CostEstimate(flops=4 * rows * width * ff, bytes_accessed=4 * width * ff, transcendentals=rows * ff),
    )


def layer_forward(hidden, w_in, w_out, layer, target=None, scale=None):
    (rows, width), ff = hidden.shape, w_in.shape[2]
    whole, in_spec, out_spec, pre_spec = layer_specs(layer, rows, width)
    bf16_rows = jax.ShapeDtypeStruct((rows, width), jnp.bfloat16)
    last = scale is not None
    return pl.pallas_call(
        functools.partial(forward_body, scale, 4),
        grid=(ff // FF_TILE,),
        out_shape=[jax.ShapeDtypeStruct((rows, ff), jnp.bfloat16), bf16_rows] if last else bf16_rows,
        in_specs=[whole, in_spec, out_spec] + ([whole] if last else []),
        out_specs=[pre_spec, whole] if last else whole,
        scratch_shapes=[pltpu.VMEM((rows, width), jnp.float32)],
        name="layer_forward",
        **layer_params(rows, width, ff),
    )(*((hidden, w_in, w_out) + ((target,) if last else ())))


def backward_body(parts, grad, pre, w_in, w_out, out, acc):
    step = pl.program_id(0)
    rows = grad.shape[0] // parts

    @pl.when(step == 0)
    def _():
        acc[...] = grad[...].astype(jnp.float32)

    for part in range(parts):
        at = pl.ds(part * rows, rows)
        e = rounded(dot_nt(grad[at], w_out[0]))
        slope = gelu_parts(pre[at].astype(jnp.float32))[1]
        acc[at] += dot_nt((slope * e).astype(jnp.bfloat16), w_in[0])

    @pl.when(step == pl.num_programs(0) - 1)
    def _():
        out[...] = acc[...].astype(jnp.bfloat16)


def layer_backward(grad, pre, w_in, w_out, layer):
    (rows, width), ff = grad.shape, w_in.shape[2]
    whole, in_spec, out_spec, pre_spec = layer_specs(layer, rows, width)
    return pl.pallas_call(
        functools.partial(backward_body, 4),
        grid=(ff // FF_TILE,),
        out_shape=jax.ShapeDtypeStruct((rows, width), jnp.bfloat16),
        in_specs=[whole, pre_spec, in_spec, out_spec],
        out_specs=whole,
        scratch_shapes=[pltpu.VMEM((rows, width), jnp.float32)],
        name="layer_backward",
        **layer_params(rows, width, ff),
    )(grad, pre, w_in, w_out)


def grads_body(count, tile, layer, bits, parts, split, *refs):
    hidden, grad = refs[:count], refs[count : 2 * count]
    w_in, w_out, out_a, out_b, hidden_buf, grad_buf, act_buf, pre_buf, window, w_in_t, w_out_buf, sem, w_sem = refs[2 * count :]
    block, width = w_in_t.shape
    span = window.shape[1]
    step, steps = pl.program_id(0), pl.num_programs(0)
    per = hidden[0].shape[0] // tile
    owner = lax.axis_index(AXIS) ^ bits
    start = jnp.minimum(owner * block // 128 * 128, w_in.shape[2] - span)
    in_copy = pltpu.make_async_copy(w_in.at[layer, :, pl.ds(pl.multiple_of(start, 128), span)], window, w_sem.at[0])
    out_copy = pltpu.make_async_copy(w_out.at[layer, pl.ds(pl.multiple_of(owner * block, 16), block)], w_out_buf, w_sem.at[1])

    def fetch(at, slot):
        for b in range(count):
            @pl.when(at // per == b)
            def _():
                rows = pl.ds(pl.multiple_of((at % per) * tile, tile), tile)
                pltpu.make_async_copy(hidden[b].at[rows], hidden_buf.at[slot], sem.at[0, slot]).start()
                pltpu.make_async_copy(grad[b].at[rows], grad_buf.at[slot], sem.at[1, slot]).start()

    slot = step % 2

    @pl.when(step == 0)
    def _():
        in_copy.start()
        out_copy.start()
        fetch(0, 0)
        in_copy.wait()
        chosen = lax.broadcasted_iota(jnp.int32, (block, span), 0) + (owner * block - start)
        chosen = (chosen == lax.broadcasted_iota(jnp.int32, (block, span), 1)).astype(jnp.bfloat16)
        w_in_t[...] = dot_nt(chosen, window[...]).astype(jnp.bfloat16)
        out_copy.wait()

    @pl.when(step + 1 < steps)
    def _():
        fetch(step + 1, 1 - slot)

    pltpu.make_async_copy(hidden[0].at[pl.ds(0, tile)], hidden_buf.at[slot], sem.at[0, slot]).wait()
    pltpu.make_async_copy(grad[0].at[pl.ds(0, tile)], grad_buf.at[slot], sem.at[1, slot]).wait()

    rows = tile // parts
    for part in range(parts):
        at = pl.ds(part * rows, rows)
        u = rounded(dot_nt(w_in_t[...], hidden_buf[slot, at]))
        e = rounded(dot_nt(w_out_buf[...], grad_buf[slot, at]))
        act, slope = gelu_parts(u)
        act_buf[:, at] = act.astype(jnp.bfloat16)
        pre_buf[:, at] = (slope * e).astype(jnp.bfloat16)
    second = dot_nn(act_buf[...], grad_buf[slot])
    first = dot_nn(pre_buf[...], hidden_buf[slot])

    half = width // 2
    pieces = (
        [(out_a, (0,), second[:, :half]), (out_b, (0,), second[:, half:]), (out_a, (1,), first[:, :half]), (out_b, (1,), first[:, half:])]
        if split
        else [(out_a, (), second), (out_b, (), first)]
    )

    @pl.when(step == 0)
    def _():
        for ref, at, value in pieces:
            ref[at + (...,)] = value

    @pl.when(step > 0)
    def _():
        for ref, at, value in pieces:
            ref[at + (...,)] += value


def column_grads(hidden, grad, w_in, w_out, layer, bits, split):
    count, width = len(hidden), hidden[0].shape[1]
    block = w_in.shape[2] // DEVICES
    span = -(-(block + 128) // 128) * 128
    tokens = count * hidden[0].shape[0]
    tile = 1024
    shape = (2, block, width // 2) if split else (block, width)
    spec = pl.BlockSpec(shape, lambda t: (0,) * len(shape))
    bf16 = jnp.bfloat16
    return pl.pallas_call(
        functools.partial(grads_body, count, tile, layer, bits, 2, split),
        grid=(tokens // tile,),
        out_shape=[jax.ShapeDtypeStruct(shape, jnp.float32)] * 2,
        in_specs=[pl.BlockSpec(memory_space=pl.ANY)] * (2 * count + 2),
        out_specs=[spec, spec],
        scratch_shapes=[pltpu.VMEM((2, tile, width), bf16)] * 2
        + [pltpu.VMEM((block, tile), bf16)] * 2
        + [pltpu.VMEM((width, span), bf16), pltpu.VMEM((block, width), bf16), pltpu.VMEM((block, width), bf16)]
        + [pltpu.SemaphoreType.DMA((2, 2)), pltpu.SemaphoreType.DMA((2,))],
        compiler_params=pltpu.CompilerParams(vmem_limit_bytes=62 * 2**20, dimension_semantics=("arbitrary",)),
        cost_estimate=pl.CostEstimate(
            flops=8 * tokens * block * width,
            bytes_accessed=4 * tokens * width + 12 * block * width,
            transcendentals=tokens * block,
        ),
        name="column_grads",
    )(*hidden, *grad, w_in, w_out)


def into_layer(body, inputs, in_specs, spec_of, grid, layer, shape, held):
    extra = [] if held is None else [held]
    return pl.pallas_call(
        functools.partial(body, len(inputs)),
        grid=grid,
        out_shape=jax.ShapeDtypeStruct(shape, jnp.float32),
        in_specs=in_specs + [pl.BlockSpec(memory_space=pl.ANY)] * len(extra),
        out_specs=spec_of(layer),
        input_output_aliases={len(inputs): 0} if extra else {},
        compiler_params=pltpu.CompilerParams(vmem_limit_bytes=48 * 2**20, dimension_semantics=("arbitrary",)),
    )(*inputs, *extra)


def sum_body(count, *refs):
    total = refs[0][...]
    for ref in refs[1:count]:
        total = total + ref[...]
    refs[-1][0] = total


def sum_into(parts, layer, layers, held):
    block, width = parts[0].shape
    rows = block // 5
    spec = pl.BlockSpec((rows, width), lambda i: (i, 0))
    return into_layer(sum_body, parts, [spec] * len(parts), lambda layer: pl.BlockSpec((1, rows, width), lambda i: (layer, i, 0)), (5,), layer, (layers, block, width), held)


def sum_halves_body(count, *refs):
    half = refs[0].shape[2]
    for side in range(2):
        mine = refs[side:count:2]
        total = mine[0][0]
        for ref in mine[1:]:
            total = total + ref[0]
        refs[-1][0, :, side * half : (side + 1) * half] = total


def sum_halves_into(pairs, layer, layers, held):
    _, block, half = pairs[0][0].shape
    rows = block // 5
    flat = [part for pair in pairs for part in pair]
    spec = pl.BlockSpec((1, rows, half), lambda i: (0, i, 0))
    return into_layer(sum_halves_body, flat, [spec] * len(flat), lambda layer: pl.BlockSpec((1, rows, 2 * half), lambda i: (layer, i, 0)), (5,), layer, (layers, block, 2 * half), held)


def turn_body(layer0, *refs):
    out = refs[-1]
    block = refs[0].shape[-2]
    for side in range(2):
        total = refs[side][...]
        for ref in refs[2 + side : layer0 : 2]:
            total = total + ref[...]
        out[side, :, :block] = total.T
        total = refs[layer0 + side][0]
        for ref in refs[layer0 + 2 + side : -1 : 2]:
            total = total + ref[0]
        out[side, :, block:] = total.T


def turn(layer0, layer1):
    block, width = layer0[0].shape
    half, step = width // 2, 256
    blocks = half // step
    low = pl.BlockSpec((block, step), lambda j: (0, j))
    high = pl.BlockSpec((block, step), lambda j: (0, blocks + j))
    part = pl.BlockSpec((1, block, step), lambda j: (1, 0, j))
    flat0 = [array for array in layer0 for _ in range(2)]
    flat1 = [array for pair in layer1 for array in pair]
    out = pl.pallas_call(
        functools.partial(turn_body, len(flat0)),
        grid=(blocks,),
        out_shape=jax.ShapeDtypeStruct((2, half, 2 * block), jnp.float32),
        in_specs=[low, high] * len(layer0) + [part] * len(flat1),
        out_specs=pl.BlockSpec((2, step, 2 * block), lambda j: (0, j, 0)),
        compiler_params=pltpu.CompilerParams(vmem_limit_bytes=48 * 2**20, dimension_semantics=("arbitrary",)),
        name="turn",
    )(*flat0, *flat1)
    return out.reshape(DEVICES, width // DEVICES, 2 * block)


def join_body(blocks, out):
    block = blocks.shape[2] // 2
    for layer in range(2):
        for i in range(blocks.shape[0]):
            out[layer, :, i * block : (i + 1) * block] = blocks[i, :, layer * block : (layer + 1) * block]


def join(blocks):
    count, rows, both = blocks.shape
    step = 32
    return pl.pallas_call(
        join_body,
        grid=(rows // step,),
        out_shape=jax.ShapeDtypeStruct((2, rows, count * both // 2), jnp.float32),
        in_specs=[pl.BlockSpec((count, step, both), lambda i: (0, i, 0))],
        out_specs=pl.BlockSpec((2, step, count * both // 2), lambda i: (0, i, 0)),
        compiler_params=pltpu.CompilerParams(vmem_limit_bytes=48 * 2**20, dimension_semantics=("arbitrary",)),
        name="join",
    )(blocks)


def solution(mesh):
    def local_grads(tokens, targets, w_in, w_out):
        layers = w_in.shape[0]
        scale = (tokens.shape[0] * DEVICES) ** -0.5

        def gather_plane(value):
            return lax.all_gather(value, AXIS, axis_index_groups=groups_of(CORE | Y | Z), tiled=True)

        def gather_pair(value):
            across = swap(value, X)
            near = swap(value, CORE)
            return [value, near, across, swap(across, CORE)]

        all_tokens = gather_plane(tokens)
        hidden1 = layer_forward(tokens, w_in, w_out, 0)
        hidden1_all = gather_pair(hidden1)
        pre1, grad1 = layer_forward(hidden1, w_in, w_out, 1, targets, scale)
        grad1_all = gather_pair(grad1)
        grad0 = layer_backward(grad1, pre1, w_in, w_out, 1)
        all_grad0 = gather_plane(grad0)

        def columns(hidden, grad, layer, bits, split):
            return column_grads(hidden, grad, w_in, w_out, layer, bits, split)

        own1 = columns(hidden1_all, grad1_all, 1, 0, True)
        far_lo, far_hi = columns(hidden1_all, grad1_all, 1, Y | Z, True)
        far_lo = swap(far_lo, Y)
        far_hi = swap(far_hi, Z)
        y_lo, y_hi = columns(hidden1_all, grad1_all, 1, Y, True)
        y_lo = swap(y_lo, Y)
        z_lo, z_hi = columns(hidden1_all, grad1_all, 1, Z, True)
        z_hi = swap(z_hi, Z)
        second0_x, first0_x = columns([all_tokens], [all_grad0], 0, X, False)
        first0_x = swap(first0_x, X)
        second0_x = swap(second0_x, X)
        y_hi = swap(y_hi + far_hi, Y)
        z_lo = swap(z_lo + far_lo, Z)
        second0, first0 = columns([all_tokens], [all_grad0], 0, 0, False)

        rows = turn([first0, first0_x], [own1, (y_lo, y_hi), (z_lo, z_hi)])
        rows = lax.all_to_all(rows, AXIS, split_axis=0, concat_axis=0, tiled=True)
        out_second = sum_halves_into([own1, (y_lo, y_hi), (z_lo, z_hi)], 1, layers, None)
        out_second = sum_into([second0, second0_x], 0, layers, out_second)
        out_first = join(rows)
        return out_first, out_second

    tok_spec = P(AXIS, None)
    grad_spec = P(None, AXIS, None)
    return jax.shard_map(local_grads, mesh=mesh, in_specs=(tok_spec, tok_spec, P(), P()), out_specs=(grad_spec, grad_spec), check_vma=False)
```

```python
import functools

import jax
import jax.numpy as jnp
from jax import lax
from jax.experimental import pallas as pl
from jax.experimental.pallas import tpu as pltpu
from jax.sharding import PartitionSpec as P


AXIS = "data"
DEVICES = 16
CORE, X, Y, Z = 1, 2, 4, 8
GELU_S = 0.7978845608028654
GELU_C = 0.044715


def swap(value, bits):
    return lax.ppermute(value, AXIS, [(i, i ^ bits) for i in range(DEVICES)])


def gelu_parts(u):
    sq = u * u
    th = jnp.tanh(u * (GELU_S + (GELU_S * GELU_C) * sq))
    cdf = 0.5 + 0.5 * th
    slope = cdf + (0.5 * u) * (1.0 - th * th) * (GELU_S + (3.0 * GELU_S * GELU_C) * sq)
    return u * cdf, slope


def rounded(value):
    return value.astype(jnp.bfloat16).astype(jnp.float32)


def dot_nn(a, b):
    return jnp.dot(a, b, preferred_element_type=jnp.float32)


def dot_nt(a, b):
    return lax.dot_general(a, b, (((1,), (1,)), ((), ())), preferred_element_type=jnp.float32)


def flipped(index, bits):
    for bit in (CORE, X, Y, Z):
        if bits & bit:
            index = index + bit - 2 * bit * (index // bit % 2)
    return index


def plane_rank(index):
    return index // Z % 2 * 4 + index // Y % 2 * 2 + index % 2


def plane_gather(own, every, send_sem, recv_sem, own_sem):
    me = lax.axis_index(AXIS)
    half = own.shape[0] // 2
    low, high = pl.ds(0, half), pl.ds(half, half)
    count = iter(range(16))

    def remote(src, dst, bits):
        n = next(count)
        return pltpu.make_async_remote_copy(
            src_ref=src, dst_ref=dst, send_sem=send_sem.at[n], recv_sem=recv_sem.at[n], device_id=(flipped(me, bits),), device_id_type=pl.DeviceIdType.MESH
        )

    def slot(bits):
        return every.at[plane_rank(flipped(me, bits))]

    def barrier():
        ready = pltpu.get_barrier_semaphore()
        for bits in (CORE, Y, Z):
            pl.semaphore_signal(ready, inc=1, device_id=(flipped(me, bits),), device_id_type=pl.DeviceIdType.MESH)
        pl.semaphore_wait(ready, 3)

    keep = pltpu.make_async_copy(own, slot(0), own_sem.at[0])
    first = [remote(own, slot(0), bits) for bits in (Y, Z, CORE)]
    from_y, from_z, far = slot(Y), slot(Z), slot(Y | Z)
    second = [
        remote(from_y.at[low], from_y.at[low], Z),
        remote(from_z.at[high], from_z.at[high], Y),
        remote(from_y, from_y, CORE),
        remote(from_z, from_z, CORE),
    ]
    last = [remote(far.at[low], far.at[low], CORE), remote(far.at[high], far.at[high], CORE)]
    return barrier, keep, first, second, last


GATHER_SEMS = [pltpu.SemaphoreType.DMA((9,)), pltpu.SemaphoreType.DMA((9,)), pltpu.SemaphoreType.DMA((1,))]


def grads_body(plan, count, outs, tile, parts, turn_at, *refs):
    arrays = refs[:count]
    w_in, w_out = refs[count : count + 2]
    own_block = arrays[-1]
    outputs = refs[count + 2 : count + 2 + outs]
    hidden_buf, grad_buf, act_buf, pre_buf, window, w_in_t, w_out_buf, acc, sem, w_sem, out_sem = refs[count + 2 + outs : count + 13 + outs]
    gather_sems = refs[count + 13 + outs :]
    block, width = w_in_t.shape
    span = window.shape[1]
    step, steps = pl.program_id(0), pl.num_programs(0)
    me = lax.axis_index(AXIS)

    begins, sources, at = [], [], 0
    for segment in plan:
        begins.append(at)
        for h, g in zip(segment["hidden"], segment["grad"]):
            tiles = arrays[h].shape[0] // tile
            sources.append((at, at + tiles, arrays[h], arrays[g]))
            at += tiles
    ends = begins[1:] + [at]
    index = sum([(step >= begin).astype(jnp.int32) for begin in begins[1:]], jnp.int32(0))
    side = index % 2
    fresh = step == begins[0]
    for begin in begins[1:]:
        fresh = fresh | (step == begin)

    def fetch(at, slot):
        for begin, end, hidden, grad in sources:
            @pl.when((at >= begin) & (at < end))
            def _():
                rows = pl.ds(pl.multiple_of((at - begin) * tile, tile), tile)
                pltpu.make_async_copy(hidden.at[rows], hidden_buf.at[slot], sem.at[0, slot]).start()
                pltpu.make_async_copy(grad.at[rows], grad_buf.at[slot], sem.at[1, slot]).start()

    def weights(k):
        segment = plan[k]
        owner = flipped(me, segment["bits"])
        start = jnp.minimum(owner * block // 128 * 128, w_in.shape[2] - span)
        return owner * block - start, (
            pltpu.make_async_copy(w_in.at[segment["layer"], :, pl.ds(pl.multiple_of(start, 128), span)], window, w_sem.at[0]),
            pltpu.make_async_copy(w_out.at[segment["layer"], pl.ds(pl.multiple_of(owner * block, 16), block)], w_out_buf.at[k % 2], w_sem.at[1]),
        )

    def results(k, which):
        out_a, out_b = outputs[2 * k : 2 * k + 2]
        if plan[k]["split"]:
            half = width // 2
            return [
                pltpu.make_async_copy(acc.at[k % 2, which, :, pl.ds(0, half)], out_a.at[which], out_sem.at[k % 2, 2 * which]),
                pltpu.make_async_copy(acc.at[k % 2, which, :, pl.ds(half, half)], out_b.at[which], out_sem.at[k % 2, 2 * which + 1]),
            ]
        return [pltpu.make_async_copy(acc.at[k % 2, which], (out_a, out_b)[which], out_sem.at[k % 2, 2 * which])]

    slot = step % 2

    @pl.when(step == 0)
    def _():
        for copy in weights(0)[1]:
            copy.start()
        fetch(0, 0)

    if turn_at is not None:
        barrier, keep, first, second, last = plane_gather(own_block, outputs[-1], *gather_sems)

        @pl.when(step == 0)
        def _():
            barrier()
            for copy in first + [keep]:
                copy.start()

        @pl.when(step == turn_at)
        def _():
            for copy in first[:2]:
                copy.wait_recv()
            for copy in second:
                copy.start()

    for k, begin in enumerate(begins):
        @pl.when(step == begin)
        def _(k=k):
            shift, copies = weights(k)
            copies[0].wait()
            chosen = lax.broadcasted_iota(jnp.int32, (block, span), 0) + shift
            chosen = (chosen == lax.broadcasted_iota(jnp.int32, (block, span), 1)).astype(jnp.bfloat16)
            w_in_t[...] = dot_nt(chosen, window[...]).astype(jnp.bfloat16)
            copies[1].wait()
            if k >= 2:
                for copy in results(k - 2, 0) + results(k - 2, 1):
                    copy.wait()

    for k, end in enumerate(ends[:-1]):
        @pl.when(step == end - 1)
        def _(k=k):
            for copy in weights(k + 1)[1]:
                copy.start()

    @pl.when(step + 1 < steps)
    def _():
        fetch(step + 1, 1 - slot)

    pltpu.make_async_copy(arrays[0].at[pl.ds(0, tile)], hidden_buf.at[slot], sem.at[0, slot]).wait()
    pltpu.make_async_copy(arrays[0].at[pl.ds(0, tile)], grad_buf.at[slot], sem.at[1, slot]).wait()

    rows = tile // parts
    for part in range(parts):
        at = pl.ds(part * rows, rows)
        u = rounded(dot_nt(w_in_t[...], hidden_buf[slot, at]))
        e = rounded(dot_nt(w_out_buf[side], grad_buf[slot, at]))
        act, slope = gelu_parts(u)
        act_buf[:, at] = act.astype(jnp.bfloat16)
        pre_buf[:, at] = (slope * e).astype(jnp.bfloat16)

    for which, left, right in ((0, act_buf, grad_buf), (1, pre_buf, hidden_buf)):
        value = dot_nn(left[...], right[slot])

        @pl.when(fresh)
        def _():
            acc[side, which] = value

        @pl.when(jnp.logical_not(fresh))
        def _():
            acc[side, which] += value

        for k, end in enumerate(ends):
            @pl.when(step == end - 1)
            def _(k=k):
                for copy in results(k, which):
                    copy.start()

    @pl.when(step == steps - 1)
    def _():
        if turn_at is not None:
            for copy in second[:2]:
                copy.wait_recv()
            for copy in last:
                copy.start()
            keep.wait()
            first[2].wait_recv()
            for copy in second[2:] + last:
                copy.wait_recv()
            for copy in first + second + last:
                copy.wait_send()
        for k in range(max(0, len(plan) - 2), len(plan)):
            for copy in results(k, 0) + results(k, 1):
                copy.wait()


def column_grads(segments, w_in, w_out, gathered=None, turn_at=None, collective_id=None):
    arrays, plan = [], []

    def place(array):
        for n, other in enumerate(arrays):
            if other is array:
                return n
        arrays.append(array)
        return len(arrays) - 1

    for hidden, grad, layer, bits, split in segments:
        plan.append(dict(hidden=[place(a) for a in hidden], grad=[place(a) for a in grad], layer=layer, bits=bits, split=split))
    width = arrays[0].shape[1]
    block = w_in.shape[2] // DEVICES
    span = -(-(block + 128) // 128) * 128
    tile = 1024
    tokens = sum(arrays[h].shape[0] for segment in plan for h in segment["hidden"])
    shapes = [(2, block, width // 2) if segment["split"] else (block, width) for segment in plan for _ in range(2)]
    out_shape = [jax.ShapeDtypeStruct(shape, jnp.float32) for shape in shapes]
    bf16 = jnp.bfloat16
    params = {}
    if gathered is not None:
        arrays.append(gathered)
        out_shape.append(jax.ShapeDtypeStruct((8,) + gathered.shape, bf16))
        params = dict(collective_id=collective_id, has_side_effects=True)
    hbm = pl.BlockSpec(memory_space=pl.ANY)
    return pl.pallas_call(
        functools.partial(grads_body, plan, len(arrays), len(out_shape), tile, 2, turn_at),
        grid=(tokens // tile,),
        out_shape=out_shape,
        in_specs=[hbm] * (len(arrays) + 2),
        out_specs=[hbm] * len(out_shape),
        scratch_shapes=[pltpu.VMEM((2, tile, width), bf16)] * 2
        + [pltpu.VMEM((block, tile), bf16)] * 2
        + [pltpu.VMEM((width, span), bf16), pltpu.VMEM((block, width), bf16), pltpu.VMEM((2, block, width), bf16)]
        + [pltpu.VMEM((2, 2, block, width), jnp.float32)]
        + [pltpu.SemaphoreType.DMA((2, 2)), pltpu.SemaphoreType.DMA((2,)), pltpu.SemaphoreType.DMA((2, 4))]
        + (GATHER_SEMS if gathered is not None else []),
        compiler_params=pltpu.CompilerParams(vmem_limit_bytes=62 * 2**20, dimension_semantics=("arbitrary",), **params),
        cost_estimate=pl.CostEstimate(
            flops=8 * tokens * block * width, bytes_accessed=4 * tokens * width + 12 * block * width * len(plan), transcendentals=tokens * block
        ),
        name="column_grads",
    )(*arrays, w_in, w_out)


FF_TILE = 1280


def pair_rank(index):
    return index // X % 2 * 2 + index % 2


def layers_body(scale, parts, tiles, *refs):
    tokens, targets, w_in, w_out, every, hidden_all, grad_all, below = refs[:8]
    now, target, acc, pre_buf, send_sem, recv_sem, own_sem, pair_send, pair_recv, local = refs[8:]
    step = pl.program_id(0)
    phase, tile = step // tiles, step % tiles
    me = lax.axis_index(AXIS)
    rows = now.shape[0] // parts
    _, keep, first, second, last = plane_gather(tokens, every, send_sem, recv_sem, own_sem)

    def remote(array, came, bits, n):
        place = array.at[pair_rank(flipped(me, came))]
        return pltpu.make_async_remote_copy(
            src_ref=place, dst_ref=place, send_sem=pair_send.at[n], recv_sem=pair_recv.at[n], device_id=(flipped(me, bits),), device_id_type=pl.DeviceIdType.MESH
        )

    def pair(array, n):
        store = pltpu.make_async_copy(now, array.at[pair_rank(me)], local.at[n])
        return store, remote(array, 0, X, 3 * n), remote(array, 0, CORE, 3 * n + 1), remote(array, X, CORE, 3 * n + 2)

    hidden_copies, grad_copies = pair(hidden_all, 0), pair(grad_all, 1)
    get_tokens = pltpu.make_async_copy(tokens, now, local.at[2])
    get_target = pltpu.make_async_copy(targets, target, local.at[3])
    put_below = pltpu.make_async_copy(now, below, local.at[4])

    def on(at):
        return pl.when(step == at)

    @on(0)
    def _():
        get_tokens.start()
        get_target.start()
        ready = pltpu.get_barrier_semaphore()
        for bits in (CORE, X, Y, Z):
            pl.semaphore_signal(ready, inc=1, device_id=(flipped(me, bits),), device_id_type=pl.DeviceIdType.MESH)
        pl.semaphore_wait(ready, 4)
        for copy in first + [keep]:
            copy.start()
        get_tokens.wait()

    @on(tiles)
    def _():
        hidden_copies[0].wait()
        hidden_copies[1].start()
        hidden_copies[2].start()

    @on(tiles + 1)
    def _():
        for copy in first[:2]:
            copy.wait_recv()
        for copy in second:
            copy.start()

    @on(2 * tiles - 1)
    def _():
        for copy in second[:2]:
            copy.wait_recv()
        for copy in last:
            copy.start()
        get_target.wait()

    @on(2 * tiles)
    def _():
        grad_copies[0].wait()
        grad_copies[1].start()
        grad_copies[2].start()
        hidden_copies[1].wait_recv()
        hidden_copies[3].start()

    @pl.when(tile == 0)
    def _():
        acc[...] = now[...].astype(jnp.float32)

    @pl.when(phase < 2)
    def _():
        for part in range(parts):
            at = pl.ds(part * rows, rows)
            pre = dot_nn(now[at], w_in[0]).astype(jnp.bfloat16)
            pre_buf[tile, at] = pre
            act = gelu_parts(pre.astype(jnp.float32))[0].astype(jnp.bfloat16)
            acc[at] += dot_nn(act, w_out[0])

    @pl.when(phase == 2)
    def _():
        for part in range(parts):
            at = pl.ds(part * rows, rows)
            e = rounded(dot_nt(now[at], w_out[0]))
            slope = gelu_parts(pre_buf[tile, at].astype(jnp.float32))[1]
            acc[at] += dot_nt((slope * e).astype(jnp.bfloat16), w_in[0])

    @on(tiles - 1)
    def _():
        now[...] = acc[...].astype(jnp.bfloat16)
        hidden_copies[0].start()

    @on(2 * tiles - 1)
    def _():
        now[...] = ((rounded(acc[...]) - target[...].astype(jnp.float32)) * scale).astype(jnp.bfloat16)
        grad_copies[0].start()

    @on(3 * tiles - 1)
    def _():
        now[...] = acc[...].astype(jnp.bfloat16)
        put_below.start()
        grad_copies[1].wait_recv()
        grad_copies[3].start()
        keep.wait()
        put_below.wait()
        first[2].wait_recv()
        for copy in second[2:] + last:
            copy.wait_recv()
        for copies in (hidden_copies, grad_copies):
            copies[2].wait_recv()
            copies[3].wait_recv()
            for copy in copies[1:]:
                copy.wait_send()
        for copy in first + second + last:
            copy.wait_send()


def run_layers(tokens, targets, w_in, w_out, scale, collective_id):
    (rows, width), ff = tokens.shape, w_in.shape[2]
    tiles = ff // FF_TILE
    bf16 = jnp.bfloat16
    hbm = pl.BlockSpec(memory_space=pl.ANY)
    return pl.pallas_call(
        functools.partial(layers_body, scale, 2, tiles),
        grid=(3 * tiles,),
        out_shape=[jax.ShapeDtypeStruct((n, rows, width), bf16) for n in (8, 4, 4)] + [jax.ShapeDtypeStruct((rows, width), bf16)],
        in_specs=[
            hbm,
            hbm,
            pl.BlockSpec((1, width, FF_TILE), lambda s: (jnp.minimum(s // tiles, 1), 0, s % tiles)),
            pl.BlockSpec((1, FF_TILE, width), lambda s: (jnp.minimum(s // tiles, 1), s % tiles, 0)),
        ],
        out_specs=[hbm] * 4,
        scratch_shapes=[
            pltpu.VMEM((rows, width), bf16),
            pltpu.VMEM((rows, width), bf16),
            pltpu.VMEM((rows, width), jnp.float32),
            pltpu.VMEM((tiles, rows, FF_TILE), bf16),
        ]
        + GATHER_SEMS
        + [pltpu.SemaphoreType.DMA((6,)), pltpu.SemaphoreType.DMA((6,)), pltpu.SemaphoreType.DMA((5,))],
        compiler_params=pltpu.CompilerParams(
            vmem_limit_bytes=62 * 2**20, dimension_semantics=("arbitrary",), collective_id=collective_id, has_side_effects=True
        ),
        cost_estimate=pl.CostEstimate(flops=12 * rows * width * ff, bytes_accessed=12 * width * ff, transcendentals=3 * rows * ff),
        name="run_layers",
    )(tokens, targets, w_in, w_out)


def into_layer(body, inputs, in_specs, spec_of, grid, layer, shape, held):
    extra = [] if held is None else [held]
    return pl.pallas_call(
        functools.partial(body, len(inputs)),
        grid=grid,
        out_shape=jax.ShapeDtypeStruct(shape, jnp.float32),
        in_specs=in_specs + [pl.BlockSpec(memory_space=pl.ANY)] * len(extra),
        out_specs=spec_of(layer),
        input_output_aliases={len(inputs): 0} if extra else {},
        compiler_params=pltpu.CompilerParams(vmem_limit_bytes=48 * 2**20, dimension_semantics=("arbitrary",)),
    )(*inputs, *extra)


def sum_body(count, *refs):
    total = refs[0][...]
    for ref in refs[1:count]:
        total = total + ref[...]
    refs[-1][0] = total


def sum_into(parts, layer, layers, held):
    block, width = parts[0].shape
    rows = block // 5
    spec = pl.BlockSpec((rows, width), lambda i: (i, 0))
    return into_layer(sum_body, parts, [spec] * len(parts), lambda layer: pl.BlockSpec((1, rows, width), lambda i: (layer, i, 0)), (5,), layer, (layers, block, width), held)


def sum_halves_body(count, *refs):
    half = refs[0].shape[2]
    for side in range(2):
        mine = refs[side:count:2]
        total = mine[0][0]
        for ref in mine[1:]:
            total = total + ref[0]
        refs[-1][0, :, side * half : (side + 1) * half] = total


def sum_halves_into(pairs, layer, layers, held):
    _, block, half = pairs[0][0].shape
    rows = block // 5
    flat = [part for pair in pairs for part in pair]
    spec = pl.BlockSpec((1, rows, half), lambda i: (0, i, 0))
    return into_layer(sum_halves_body, flat, [spec] * len(flat), lambda layer: pl.BlockSpec((1, rows, 2 * half), lambda i: (layer, i, 0)), (5,), layer, (layers, block, 2 * half), held)


def turn_body(layer0, *refs):
    out = refs[-1]
    block = refs[0].shape[-2]
    for side in range(2):
        total = refs[side][...]
        for ref in refs[2 + side : layer0 : 2]:
            total = total + ref[...]
        out[side, :, :block] = total.T
        total = refs[layer0 + side][0]
        for ref in refs[layer0 + 2 + side : -1 : 2]:
            total = total + ref[0]
        out[side, :, block:] = total.T


def turn(layer0, layer1):
    block, width = layer0[0].shape
    half, step = width // 2, 256
    blocks = half // step
    low = pl.BlockSpec((block, step), lambda j: (0, j))
    high = pl.BlockSpec((block, step), lambda j: (0, blocks + j))
    part = pl.BlockSpec((1, block, step), lambda j: (1, 0, j))
    flat0 = [array for array in layer0 for _ in range(2)]
    flat1 = [array for pair in layer1 for array in pair]
    out = pl.pallas_call(
        functools.partial(turn_body, len(flat0)),
        grid=(blocks,),
        out_shape=jax.ShapeDtypeStruct((2, half, 2 * block), jnp.float32),
        in_specs=[low, high] * len(layer0) + [part] * len(flat1),
        out_specs=pl.BlockSpec((2, step, 2 * block), lambda j: (0, j, 0)),
        compiler_params=pltpu.CompilerParams(vmem_limit_bytes=48 * 2**20, dimension_semantics=("arbitrary",)),
        name="turn",
    )(*flat0, *flat1)
    return out.reshape(DEVICES, width // DEVICES, 2 * block)


def join_body(blocks, out):
    block = blocks.shape[2] // 2
    for layer in range(2):
        for i in range(blocks.shape[0]):
            out[layer, :, i * block : (i + 1) * block] = blocks[i, :, layer * block : (layer + 1) * block]


def join(blocks):
    count, rows, both = blocks.shape
    step = 32
    return pl.pallas_call(
        join_body,
        grid=(rows // step,),
        out_shape=jax.ShapeDtypeStruct((2, rows, count * both // 2), jnp.float32),
        in_specs=[pl.BlockSpec((count, step, both), lambda i: (0, i, 0))],
        out_specs=pl.BlockSpec((2, step, count * both // 2), lambda i: (0, i, 0)),
        compiler_params=pltpu.CompilerParams(vmem_limit_bytes=48 * 2**20, dimension_semantics=("arbitrary",)),
        name="join",
    )(blocks)


def solution(mesh):
    def local_grads(tokens, targets, w_in, w_out):
        layers = w_in.shape[0]
        scale = (tokens.shape[0] * DEVICES) ** -0.5

        all_tokens, hidden1_all, grad1_all, grad0 = run_layers(tokens, targets, w_in, w_out, scale, 1)
        all_tokens, hidden1_all, grad1_all = (array.reshape(-1, tokens.shape[1]) for array in (all_tokens, hidden1_all, grad1_all))
        hidden1_all, grad1_all = [hidden1_all], [grad1_all]

        far_lo, far_hi, y_lo, y_hi, z_lo, z_hi, all_grad0 = column_grads(
            [(hidden1_all, grad1_all, 1, bits, True) for bits in (Y | Z, Y, Z)], w_in, w_out, grad0, 8, 0
        )
        all_grad0 = all_grad0.reshape(all_tokens.shape)
        far_lo = swap(far_lo, Y)
        far_hi = swap(far_hi, Z)
        y_lo = swap(y_lo, Y)
        z_hi = swap(z_hi, Z)
        second0_x, first0_x = column_grads([([all_tokens], [all_grad0], 0, X, False)], w_in, w_out)
        first0_x = swap(first0_x, X)
        second0_x = swap(second0_x, X)
        y_hi = swap(y_hi + far_hi, Y)
        z_lo = swap(z_lo + far_lo, Z)
        *own1, second0, first0 = column_grads([(hidden1_all, grad1_all, 1, 0, True), ([all_tokens], [all_grad0], 0, 0, False)], w_in, w_out)

        rows = turn([first0, first0_x], [own1, (y_lo, y_hi), (z_lo, z_hi)])
        rows = lax.all_to_all(rows, AXIS, split_axis=0, concat_axis=0, tiled=True)
        out_second = sum_halves_into([own1, (y_lo, y_hi), (z_lo, z_hi)], 1, layers, None)
        out_second = sum_into([second0, second0_x], 0, layers, out_second)
        out_first = join(rows)
        return out_first, out_second

    tok_spec = P(AXIS, None)
    grad_spec = P(None, AXIS, None)
    return jax.shard_map(local_grads, mesh=mesh, in_specs=(tok_spec, tok_spec, P(), P()), out_specs=(grad_spec, grad_spec), check_vma=False)
```

```python
import functools

import jax
import jax.numpy as jnp
from jax import lax
from jax.experimental import pallas as pl
from jax.experimental.pallas import tpu as pltpu
from jax.sharding import PartitionSpec as P


AXIS = "data"
DEVICES = 16
CORE, X, Y, Z = 1, 2, 4, 8
GELU_S = 0.7978845608028654
GELU_C = 0.044715


def swap(value, bits):
    return lax.ppermute(value, AXIS, [(i, i ^ bits) for i in range(DEVICES)])


def gelu_parts(u):
    sq = u * u
    th = jnp.tanh(u * (GELU_S + (GELU_S * GELU_C) * sq))
    cdf = 0.5 + 0.5 * th
    slope = cdf + (0.5 * u) * (1.0 - th * th) * (GELU_S + (3.0 * GELU_S * GELU_C) * sq)
    return u * cdf, slope


def rounded(value):
    return value.astype(jnp.bfloat16).astype(jnp.float32)


def dot_nn(a, b):
    return jnp.dot(a, b, preferred_element_type=jnp.float32)


def dot_nt(a, b):
    return lax.dot_general(a, b, (((1,), (1,)), ((), ())), preferred_element_type=jnp.float32)


def flipped(index, bits):
    for bit in (CORE, X, Y, Z):
        if bits & bit:
            index = index + bit - 2 * bit * (index // bit % 2)
    return index


def pair_rank(index):
    return index // X % 2 * 2 + index % 2


def plane_rank(index):
    return index // Z % 2 * 4 + index // Y % 2 * 2 + index % 2


def plane_gather(own, every, send_sem, recv_sem, own_sem):
    me = lax.axis_index(AXIS)
    half = own.shape[0] // 2
    low, high = pl.ds(0, half), pl.ds(half, half)
    count = iter(range(16))

    def remote(src, dst, bits):
        n = next(count)
        return pltpu.make_async_remote_copy(
            src_ref=src, dst_ref=dst, send_sem=send_sem.at[n], recv_sem=recv_sem.at[n], device_id=(flipped(me, bits),), device_id_type=pl.DeviceIdType.MESH
        )

    def slot(bits):
        return every.at[plane_rank(flipped(me, bits))]

    def barrier():
        ready = pltpu.get_barrier_semaphore()
        for bits in (CORE, Y, Z):
            pl.semaphore_signal(ready, inc=1, device_id=(flipped(me, bits),), device_id_type=pl.DeviceIdType.MESH)
        pl.semaphore_wait(ready, 3)

    keep = pltpu.make_async_copy(own, slot(0), own_sem.at[0])
    first = [remote(own, slot(0), bits) for bits in (Y, Z, CORE)]
    from_y, from_z, far = slot(Y), slot(Z), slot(Y | Z)
    second = [
        remote(from_y.at[low], from_y.at[low], Z),
        remote(from_z.at[high], from_z.at[high], Y),
        remote(from_y, from_y, CORE),
        remote(from_z, from_z, CORE),
    ]
    last = [remote(far.at[low], far.at[low], CORE), remote(far.at[high], far.at[high], CORE)]
    return barrier, keep, first, second, last


GATHER_SEMS = [pltpu.SemaphoreType.DMA((9,)), pltpu.SemaphoreType.DMA((9,)), pltpu.SemaphoreType.DMA((1,))]


def grads_body(plan, count, outs, tile, parts, turn_at, late, *refs):
    arrays = list(refs[:count])
    w_in, w_out = refs[count : count + 2]
    own_block = arrays[-1]
    outputs = refs[count + 2 : count + 2 + outs]
    hidden_buf, grad_buf, act_buf, pre_buf, window, w_in_t, w_out_buf, acc, sem, w_sem, out_sem = refs[count + 2 + outs : count + 13 + outs]
    if late is not None:
        arrays[late] = outputs[-1]
    gather_sems = refs[count + 13 + outs :]
    block, width = w_in_t.shape
    span = window.shape[1]
    step, steps = pl.program_id(0), pl.num_programs(0)
    me = lax.axis_index(AXIS)

    begins, sources, at = [], [], 0
    for segment in plan:
        begins.append(at)
        for h, g in zip(segment["hidden"], segment["grad"]):
            tiles = arrays[h].shape[0] // tile
            sources.append((at, at + tiles, arrays[h], arrays[g], segment["layer"]))
            at += tiles
    ends = begins[1:] + [at]
    index = sum([(step >= begin).astype(jnp.int32) for begin in begins[1:]], jnp.int32(0))
    side = index % 2
    fresh = step == begins[0]
    for begin in begins[1:]:
        fresh = fresh | (step == begin)

    def fetch(at, slot):
        for begin, end, hidden, grad, layer in sources:
            @pl.when((at >= begin) & (at < end))
            def _():
                place = at - begin
                if layer == 1:
                    place = (me // X + place // 2) % 2 * 2 + (me + place) % 2
                rows = pl.ds(pl.multiple_of(place * tile, tile), tile)
                pltpu.make_async_copy(hidden.at[rows], hidden_buf.at[slot], sem.at[0, slot]).start()
                pltpu.make_async_copy(grad.at[rows], grad_buf.at[slot], sem.at[1, slot]).start()

    def weights(k):
        segment = plan[k]
        owner = flipped(me, segment["bits"])
        start = jnp.minimum(owner * block // 128 * 128, w_in.shape[2] - span)
        return owner * block - start, (
            pltpu.make_async_copy(w_in.at[segment["layer"], :, pl.ds(pl.multiple_of(start, 128), span)], window, w_sem.at[0]),
            pltpu.make_async_copy(w_out.at[segment["layer"], pl.ds(pl.multiple_of(owner * block, 16), block)], w_out_buf.at[k % 2], w_sem.at[1]),
        )

    def results(k, which):
        out_a, out_b = outputs[2 * k : 2 * k + 2]
        if plan[k]["split"]:
            half = width // 2
            return [
                pltpu.make_async_copy(acc.at[k % 2, which, :, pl.ds(0, half)], out_a.at[which], out_sem.at[k % 2, 2 * which]),
                pltpu.make_async_copy(acc.at[k % 2, which, :, pl.ds(half, half)], out_b.at[which], out_sem.at[k % 2, 2 * which + 1]),
            ]
        return [pltpu.make_async_copy(acc.at[k % 2, which], (out_a, out_b)[which], out_sem.at[k % 2, 2 * which])]

    slot = step % 2

    @pl.when(step == 0)
    def _():
        for copy in weights(0)[1]:
            copy.start()
        fetch(0, 0)

    if turn_at is not None:
        barrier, keep, first, second, last = plane_gather(own_block, outputs[-2], *gather_sems[:3])
        far = arrays[late].at[pl.ds(pl.multiple_of(pair_rank(flipped(me, X)) * tile, tile), tile)]
        far_copy = pltpu.make_async_remote_copy(
            src_ref=far, dst_ref=far, send_sem=gather_sems[3].at[0], recv_sem=gather_sems[3].at[1], device_id=(flipped(me, CORE),), device_id_type=pl.DeviceIdType.MESH
        )

        @pl.when(step == 0)
        def _():
            barrier()
            for copy in first + [keep, far_copy]:
                copy.start()

        @pl.when(step == 2)
        def _():
            far_copy.wait_recv()

        @pl.when(step == turn_at)
        def _():
            for copy in first[:2]:
                copy.wait_recv()
            for copy in second:
                copy.start()

    @pl.when(fresh)
    def _():
        copies = weights(0)[1]
        copies[0].wait()
        shift = weights(0)[0]
        for k in range(1, len(plan)):
            shift = jnp.where(index == k, weights(k)[0], shift)
        chosen = lax.broadcasted_iota(jnp.int32, (block, span), 0) + shift
        chosen = (chosen == lax.broadcasted_iota(jnp.int32, (block, span), 1)).astype(jnp.bfloat16)
        w_in_t[...] = dot_nt(chosen, window[...]).astype(jnp.bfloat16)
        copies[1].wait()

    for k in range(2, len(plan)):
        @pl.when(step == begins[k])
        def _(k=k):
            for copy in results(k - 2, 0) + results(k - 2, 1):
                copy.wait()

    for k, end in enumerate(ends[:-1]):
        @pl.when(step == end - 1)
        def _(k=k):
            for copy in weights(k + 1)[1]:
                copy.start()

    @pl.when(step + 1 < steps)
    def _():
        fetch(step + 1, 1 - slot)

    pltpu.make_async_copy(arrays[0].at[pl.ds(0, tile)], hidden_buf.at[slot], sem.at[0, slot]).wait()
    pltpu.make_async_copy(arrays[0].at[pl.ds(0, tile)], grad_buf.at[slot], sem.at[1, slot]).wait()

    rows = tile // parts
    for part in range(parts):
        at = pl.ds(part * rows, rows)
        u = rounded(dot_nt(w_in_t[...], hidden_buf[slot, at]))
        e = rounded(dot_nt(w_out_buf[side], grad_buf[slot, at]))
        act, slope = gelu_parts(u)
        act_buf[:, at] = act.astype(jnp.bfloat16)
        pre_buf[:, at] = (slope * e).astype(jnp.bfloat16)

    for which, left, right in ((0, act_buf, grad_buf), (1, pre_buf, hidden_buf)):
        value = dot_nn(left[...], right[slot])

        @pl.when(fresh)
        def _():
            acc[side, which] = value

        @pl.when(jnp.logical_not(fresh))
        def _():
            acc[side, which] += value

        for k, end in enumerate(ends):
            @pl.when(step == end - 1)
            def _(k=k):
                for copy in results(k, which):
                    copy.start()

    @pl.when(step == steps - 1)
    def _():
        if turn_at is not None:
            for copy in second[:2]:
                copy.wait_recv()
            for copy in last:
                copy.start()
            keep.wait()
            first[2].wait_recv()
            for copy in second[2:] + last:
                copy.wait_recv()
            for copy in first + second + last + [far_copy]:
                copy.wait_send()
        for k in range(max(0, len(plan) - 2), len(plan)):
            for copy in results(k, 0) + results(k, 1):
                copy.wait()


def column_grads(segments, w_in, w_out, gathered=None, turn_at=None, unfinished=None, collective_id=None):
    arrays, plan = [], []

    def place(array):
        for n, other in enumerate(arrays):
            if other is array:
                return n
        arrays.append(array)
        return len(arrays) - 1

    for hidden, grad, layer, bits, split in segments:
        plan.append(dict(hidden=[place(a) for a in hidden], grad=[place(a) for a in grad], layer=layer, bits=bits, split=split))
    width = arrays[0].shape[1]
    block = w_in.shape[2] // DEVICES
    span = -(-(block + 128) // 128) * 128
    tile = 1024
    tokens = sum(arrays[h].shape[0] for segment in plan for h in segment["hidden"])
    shapes = [(2, block, width // 2) if segment["split"] else (block, width) for segment in plan for _ in range(2)]
    out_shape = [jax.ShapeDtypeStruct(shape, jnp.float32) for shape in shapes]
    bf16 = jnp.bfloat16
    params, late, aliases = {}, None, {}
    if gathered is not None:
        late = place(unfinished)
        arrays.append(gathered)
        out_shape.append(jax.ShapeDtypeStruct((8,) + gathered.shape, bf16))
        out_shape.append(jax.ShapeDtypeStruct(unfinished.shape, bf16))
        aliases = {late: len(out_shape) - 1}
        params = dict(collective_id=collective_id, has_side_effects=True)
    hbm = pl.BlockSpec(memory_space=pl.ANY)
    return pl.pallas_call(
        functools.partial(grads_body, plan, len(arrays), len(out_shape), tile, 2, turn_at, late),
        grid=(tokens // tile,),
        out_shape=out_shape,
        in_specs=[hbm] * (len(arrays) + 2),
        out_specs=[hbm] * len(out_shape),
        scratch_shapes=[pltpu.VMEM((2, tile, width), bf16)] * 2
        + [pltpu.VMEM((block, tile), bf16)] * 2
        + [pltpu.VMEM((width, span), bf16), pltpu.VMEM((block, width), bf16), pltpu.VMEM((2, block, width), bf16)]
        + [pltpu.VMEM((2, 2, block, width), jnp.float32)]
        + [pltpu.SemaphoreType.DMA((2, 2)), pltpu.SemaphoreType.DMA((2,)), pltpu.SemaphoreType.DMA((2, 4))]
        + (GATHER_SEMS + [pltpu.SemaphoreType.DMA((2,))] if gathered is not None else []),
        input_output_aliases=aliases,
        compiler_params=pltpu.CompilerParams(vmem_limit_bytes=62 * 2**20, dimension_semantics=("arbitrary",), **params),
        cost_estimate=pl.CostEstimate(
            flops=8 * tokens * block * width, bytes_accessed=4 * tokens * width + 12 * block * width * len(plan), transcendentals=tokens * block
        ),
        name="column_grads",
    )(*arrays, w_in, w_out)


FF_TILE = 1280


def layers_body(scale, parts, tiles, *refs):
    tokens, targets, w_in, w_out, every, hidden_all, grad_all, below = refs[:8]
    now, target, acc, pre_buf, send_sem, recv_sem, own_sem, pair_send, pair_recv, local = refs[8:]
    step = pl.program_id(0)
    phase, tile = step // tiles, step % tiles
    me = lax.axis_index(AXIS)
    rows = now.shape[0] // parts
    _, keep, first, second, last = plane_gather(tokens, every, send_sem, recv_sem, own_sem)

    def remote(array, came, bits, n):
        place = array.at[pair_rank(flipped(me, came))]
        return pltpu.make_async_remote_copy(
            src_ref=place, dst_ref=place, send_sem=pair_send.at[n], recv_sem=pair_recv.at[n], device_id=(flipped(me, bits),), device_id_type=pl.DeviceIdType.MESH
        )

    def pair(array, n):
        store = pltpu.make_async_copy(now, array.at[pair_rank(me)], local.at[n])
        return store, remote(array, 0, X, 3 * n), remote(array, 0, CORE, 3 * n + 1)

    hidden_copies, grad_copies = pair(hidden_all, 0) + (remote(hidden_all, X, CORE, 2),), pair(grad_all, 1)
    get_tokens = pltpu.make_async_copy(tokens, now, local.at[2])
    get_target = pltpu.make_async_copy(targets, target, local.at[3])
    put_below = pltpu.make_async_copy(now, below, local.at[4])

    def on(at):
        return pl.when(step == at)

    @on(0)
    def _():
        get_tokens.start()
        get_target.start()
        ready = pltpu.get_barrier_semaphore()
        for bits in (CORE, X, Y, Z):
            pl.semaphore_signal(ready, inc=1, device_id=(flipped(me, bits),), device_id_type=pl.DeviceIdType.MESH)
        pl.semaphore_wait(ready, 4)
        for copy in first + [keep]:
            copy.start()
        get_tokens.wait()

    @on(tiles)
    def _():
        hidden_copies[0].wait()
        hidden_copies[1].start()
        hidden_copies[2].start()

    @on(tiles + 1)
    def _():
        for copy in first[:2]:
            copy.wait_recv()
        for copy in second:
            copy.start()

    @on(2 * tiles - 1)
    def _():
        for copy in second[:2]:
            copy.wait_recv()
        for copy in last:
            copy.start()
        get_target.wait()

    @on(2 * tiles)
    def _():
        grad_copies[0].wait()
        grad_copies[1].start()
        grad_copies[2].start()
        hidden_copies[1].wait_recv()
        hidden_copies[3].start()

    @pl.when(tile == 0)
    def _():
        acc[...] = now[...].astype(jnp.float32)

    @pl.when(phase < 2)
    def _():
        for part in range(parts):
            at = pl.ds(part * rows, rows)
            pre = dot_nn(now[at], w_in[0]).astype(jnp.bfloat16)
            pre_buf[tile, at] = pre
            act = gelu_parts(pre.astype(jnp.float32))[0].astype(jnp.bfloat16)
            acc[at] += dot_nn(act, w_out[0])

    @pl.when(phase == 2)
    def _():
        for part in range(parts):
            at = pl.ds(part * rows, rows)
            e = rounded(dot_nt(now[at], w_out[0]))
            slope = gelu_parts(pre_buf[tile, at].astype(jnp.float32))[1]
            acc[at] += dot_nt((slope * e).astype(jnp.bfloat16), w_in[0])

    @on(tiles - 1)
    def _():
        now[...] = acc[...].astype(jnp.bfloat16)
        hidden_copies[0].start()

    @on(2 * tiles - 1)
    def _():
        now[...] = ((rounded(acc[...]) - target[...].astype(jnp.float32)) * scale).astype(jnp.bfloat16)
        grad_copies[0].start()

    @on(3 * tiles - 1)
    def _():
        now[...] = acc[...].astype(jnp.bfloat16)
        put_below.start()
        grad_copies[1].wait_recv()
        keep.wait()
        put_below.wait()
        first[2].wait_recv()
        for copy in second[2:] + last:
            copy.wait_recv()
        for copy in hidden_copies[2:] + grad_copies[2:3]:
            copy.wait_recv()
        for copy in hidden_copies[1:] + grad_copies[1:3]:
            copy.wait_send()
        for copy in first + second + last:
            copy.wait_send()


def run_layers(tokens, targets, w_in, w_out, scale, collective_id):
    (rows, width), ff = tokens.shape, w_in.shape[2]
    tiles = ff // FF_TILE
    bf16 = jnp.bfloat16
    hbm = pl.BlockSpec(memory_space=pl.ANY)
    return pl.pallas_call(
        functools.partial(layers_body, scale, 2, tiles),
        grid=(3 * tiles,),
        out_shape=[jax.ShapeDtypeStruct((n, rows, width), bf16) for n in (8, 4, 4)] + [jax.ShapeDtypeStruct((rows, width), bf16)],
        in_specs=[
            hbm,
            hbm,
            pl.BlockSpec((1, width, FF_TILE), lambda s: (jnp.minimum(s // tiles, 1), 0, s % tiles)),
            pl.BlockSpec((1, FF_TILE, width), lambda s: (jnp.minimum(s // tiles, 1), s % tiles, 0)),
        ],
        out_specs=[hbm] * 4,
        scratch_shapes=[
            pltpu.VMEM((rows, width), bf16),
            pltpu.VMEM((rows, width), bf16),
            pltpu.VMEM((rows, width), jnp.float32),
            pltpu.VMEM((tiles, rows, FF_TILE), bf16),
        ]
        + GATHER_SEMS
        + [pltpu.SemaphoreType.DMA((6,)), pltpu.SemaphoreType.DMA((6,)), pltpu.SemaphoreType.DMA((5,))],
        compiler_params=pltpu.CompilerParams(
            vmem_limit_bytes=62 * 2**20, dimension_semantics=("arbitrary",), collective_id=collective_id, has_side_effects=True
        ),
        cost_estimate=pl.CostEstimate(flops=12 * rows * width * ff, bytes_accessed=12 * width * ff, transcendentals=3 * rows * ff),
        name="run_layers",
    )(tokens, targets, w_in, w_out)


def into_layer(body, inputs, in_specs, spec_of, grid, layer, shape, held):
    extra = [] if held is None else [held]
    return pl.pallas_call(
        functools.partial(body, len(inputs)),
        grid=grid,
        out_shape=jax.ShapeDtypeStruct(shape, jnp.float32),
        in_specs=in_specs + [pl.BlockSpec(memory_space=pl.ANY)] * len(extra),
        out_specs=spec_of(layer),
        input_output_aliases={len(inputs): 0} if extra else {},
        compiler_params=pltpu.CompilerParams(vmem_limit_bytes=62 * 2**20, dimension_semantics=("arbitrary",)),
    )(*inputs, *extra)


def sum_body(count, *refs):
    total = refs[0][...]
    for ref in refs[1:count]:
        total = total + ref[...]
    refs[-1][0] = total


def sum_into(parts, layer, layers, held):
    block, width = parts[0].shape
    rows = block // 5
    spec = pl.BlockSpec((rows, width), lambda i: (i, 0))
    return into_layer(sum_body, parts, [spec] * len(parts), lambda layer: pl.BlockSpec((1, rows, width), lambda i: (layer, i, 0)), (5,), layer, (layers, block, width), held)


def sum_halves_body(count, *refs):
    half = refs[0].shape[2]
    for side in range(2):
        mine = refs[side:count:2]
        total = mine[0][0]
        for ref in mine[1:]:
            total = total + ref[0]
        refs[-1][0, :, side * half : (side + 1) * half] = total


def sum_halves_into(pairs, layer, layers, held):
    _, block, half = pairs[0][0].shape
    rows = block // 5
    flat = [part for pair in pairs for part in pair]
    spec = pl.BlockSpec((1, rows, half), lambda i: (0, i, 0))
    return into_layer(sum_halves_body, flat, [spec] * len(flat), lambda layer: pl.BlockSpec((1, rows, 2 * half), lambda i: (layer, i, 0)), (5,), layer, (layers, block, 2 * half), held)


def turn_body(lead, *refs):
    for side in range(2):
        total = refs[side][lead]
        for ref in refs[2 + side : -1 : 2]:
            total = total + ref[lead]
        refs[-1][side] = total.T


def turn(parts):
    pairs = isinstance(parts[0], (list, tuple))
    block, half = (parts[0][0].shape if pairs else parts[0].shape)[-2:]
    half = half if pairs else half // 2
    step = 256
    blocks = half // step
    if pairs:
        specs = [pl.BlockSpec((1, block, step), lambda j: (1, 0, j))] * 2
        flat = [array for pair in parts for array in pair]
    else:
        specs = [pl.BlockSpec((block, step), lambda j: (0, j)), pl.BlockSpec((block, step), lambda j: (0, blocks + j))]
        flat = [array for array in parts for _ in range(2)]
    out = pl.pallas_call(
        functools.partial(turn_body, 0 if pairs else slice(None)),
        grid=(blocks,),
        out_shape=jax.ShapeDtypeStruct((2, half, block), jnp.float32),
        in_specs=specs * len(parts),
        out_specs=pl.BlockSpec((2, step, block), lambda j: (0, j, 0)),
        compiler_params=pltpu.CompilerParams(vmem_limit_bytes=62 * 2**20, dimension_semantics=("arbitrary",)),
    )(*flat)
    return out.reshape(DEVICES, 2 * half // DEVICES, block)


def join_body(count, blocks, *refs):
    out = refs[-1]
    block = blocks.shape[2]
    for i in range(blocks.shape[0]):
        out[0, :, i * block : (i + 1) * block] = blocks[i]


def join_into(blocks, layer, layers, held):
    count, rows, block = blocks.shape
    step = 32
    in_spec = pl.BlockSpec((count, step, block), lambda i: (0, i, 0))
    return into_layer(
        join_body, [blocks], [in_spec], lambda layer: pl.BlockSpec((1, step, count * block), lambda i: (layer, i, 0)), (rows // step,), layer, (layers, rows, count * block), held
    )


def solution(mesh):
    def local_grads(tokens, targets, w_in, w_out):
        layers = w_in.shape[0]
        scale = (tokens.shape[0] * DEVICES) ** -0.5

        all_tokens, hidden1_all, grad1_all, grad0 = run_layers(tokens, targets, w_in, w_out, scale, 1)
        all_tokens, hidden1_all, grad1_all = (array.reshape(-1, tokens.shape[1]) for array in (all_tokens, hidden1_all, grad1_all))
        hidden1_all = [hidden1_all]

        far_lo, far_hi, y_lo, y_hi, z_lo, z_hi, all_grad0, grad1_all = column_grads(
            [(hidden1_all, [grad1_all], 1, bits, True) for bits in (Y | Z, Y, Z)], w_in, w_out, grad0, 8, grad1_all, 0
        )
        grad1_all = [grad1_all]
        all_grad0 = all_grad0.reshape(all_tokens.shape)
        far_lo = swap(far_lo, Y)
        far_hi = swap(far_hi, Z)
        y_lo = swap(y_lo, Y)
        z_hi = swap(z_hi, Z)
        second0_x, first0_x = column_grads([([all_tokens], [all_grad0], 0, X, False)], w_in, w_out)
        first0_x = swap(first0_x, X)
        second0_x = swap(second0_x, X)
        y_hi = swap(y_hi + far_hi, Y)
        z_lo = swap(z_lo + far_lo, Z)
        *own1, second0, first0 = column_grads([(hidden1_all, grad1_all, 1, 0, True), ([all_tokens], [all_grad0], 0, 0, False)], w_in, w_out)

        def exchange(first):
            return lax.all_to_all(first, AXIS, split_axis=0, concat_axis=0, tiled=True)

        first0 = turn([first0, first0_x])
        first0 = exchange(first0)
        first1 = turn([own1, (y_lo, y_hi), (z_lo, z_hi)])
        first1 = exchange(first1)
        out_second = sum_halves_into([own1, (y_lo, y_hi), (z_lo, z_hi)], 1, layers, None)
        out_second = sum_into([second0, second0_x], 0, layers, out_second)
        out_first = join_into(first0, 0, layers, None)
        out_first = join_into(first1, 1, layers, out_first)
        return out_first, out_second

    tok_spec = P(AXIS, None)
    grad_spec = P(None, AXIS, None)
    return jax.shard_map(local_grads, mesh=mesh, in_specs=(tok_spec, tok_spec, P(), P()), out_specs=(grad_spec, grad_spec), check_vma=False)
```

```python
import functools

import jax
import jax.numpy as jnp
from jax import lax
from jax.experimental import pallas as pl
from jax.experimental.pallas import tpu as pltpu
from jax.sharding import PartitionSpec as P


AXIS = "data"
DEVICES = 16
CORE, X, Y, Z = 1, 2, 4, 8
GELU_S = 0.7978845608028654
GELU_C = 0.044715


def swap(value, bits):
    return lax.ppermute(value, AXIS, [(i, i ^ bits) for i in range(DEVICES)])


def gelu_parts(u):
    sq = u * u
    th = jnp.tanh(u * (GELU_S + (GELU_S * GELU_C) * sq))
    cdf = 0.5 + 0.5 * th
    slope = cdf + (0.5 * u) * (1.0 - th * th) * (GELU_S + (3.0 * GELU_S * GELU_C) * sq)
    return u * cdf, slope


def rounded(value):
    return value.astype(jnp.bfloat16).astype(jnp.float32)


def dot_nn(a, b):
    return jnp.dot(a, b, preferred_element_type=jnp.float32)


def dot_nt(a, b):
    return lax.dot_general(a, b, (((1,), (1,)), ((), ())), preferred_element_type=jnp.float32)


def flipped(index, bits):
    for bit in (CORE, X, Y, Z):
        if bits & bit:
            index = index + bit - 2 * bit * (index // bit % 2)
    return index


def pair_rank(index):
    return index // X % 2 * 2 + index % 2


def plane_rank(index):
    return index // Z % 2 * 4 + index // Y % 2 * 2 + index % 2


def plane_gather(own, every, send_sem, recv_sem, own_sem):
    me = lax.axis_index(AXIS)
    half = own.shape[0] // 2
    low, high = pl.ds(0, half), pl.ds(half, half)
    count = iter(range(16))

    def remote(src, dst, bits):
        n = next(count)
        return pltpu.make_async_remote_copy(
            src_ref=src, dst_ref=dst, send_sem=send_sem.at[n], recv_sem=recv_sem.at[n], device_id=(flipped(me, bits),), device_id_type=pl.DeviceIdType.MESH
        )

    def slot(bits):
        return every.at[plane_rank(flipped(me, bits))]

    def barrier():
        ready = pltpu.get_barrier_semaphore()
        for bits in (CORE, Y, Z):
            pl.semaphore_signal(ready, inc=1, device_id=(flipped(me, bits),), device_id_type=pl.DeviceIdType.MESH)
        pl.semaphore_wait(ready, 3)

    keep = pltpu.make_async_copy(own, slot(0), own_sem.at[0])
    first = [remote(own, slot(0), bits) for bits in (Y, Z, CORE)]
    from_y, from_z, far = slot(Y), slot(Z), slot(Y | Z)
    second = [
        remote(from_y.at[low], from_y.at[low], Z),
        remote(from_z.at[high], from_z.at[high], Y),
        remote(from_y, from_y, CORE),
        remote(from_z, from_z, CORE),
    ]
    last = [remote(far.at[low], far.at[low], CORE), remote(far.at[high], far.at[high], CORE)]
    return barrier, keep, first, second, last


GATHER_SEMS = [pltpu.SemaphoreType.DMA((9,)), pltpu.SemaphoreType.DMA((9,)), pltpu.SemaphoreType.DMA((1,))]


def grads_body(plan, count, outs, tile, parts, turn_at, late, *refs):
    arrays = list(refs[:count])
    w_in, w_out = refs[count : count + 2]
    own_block = arrays[-1]
    outputs = refs[count + 2 : count + 2 + outs]
    hidden_buf, grad_buf, act_buf, pre_buf, window, w_in_t, w_out_buf, acc, sem, w_sem, out_sem = refs[count + 2 + outs : count + 13 + outs]
    if late is not None:
        arrays[late] = outputs[-1]
    gather_sems = refs[count + 13 + outs :]
    block, width = w_in_t.shape
    span = window.shape[1]
    step, steps = pl.program_id(0), pl.num_programs(0)
    me = lax.axis_index(AXIS)

    begins, sources, at = [], [], 0
    for segment in plan:
        begins.append(at)
        for h, g in zip(segment["hidden"], segment["grad"]):
            tiles = arrays[h].shape[0] // tile
            sources.append((at, at + tiles, arrays[h], arrays[g], segment["layer"]))
            at += tiles
    ends = begins[1:] + [at]
    index = sum([(step >= begin).astype(jnp.int32) for begin in begins[1:]], jnp.int32(0))
    side = index % 2
    fresh = step == begins[0]
    for begin in begins[1:]:
        fresh = fresh | (step == begin)

    def fetch(at, slot):
        for begin, end, hidden, grad, layer in sources:
            @pl.when((at >= begin) & (at < end))
            def _():
                place = at - begin
                if layer == 1:
                    place = (me // X + place // 2) % 2 * 2 + (me + place) % 2
                rows = pl.ds(pl.multiple_of(place * tile, tile), tile)
                pltpu.make_async_copy(hidden.at[rows], hidden_buf.at[slot], sem.at[0, slot]).start()
                pltpu.make_async_copy(grad.at[rows], grad_buf.at[slot], sem.at[1, slot]).start()

    def weights(k):
        segment = plan[k]
        owner = flipped(me, segment["bits"])
        start = jnp.minimum(owner * block // 128 * 128, w_in.shape[2] - span)
        return owner * block - start, (
            pltpu.make_async_copy(w_in.at[segment["layer"], :, pl.ds(pl.multiple_of(start, 128), span)], window, w_sem.at[0]),
            pltpu.make_async_copy(w_out.at[segment["layer"], pl.ds(pl.multiple_of(owner * block, 16), block)], w_out_buf.at[k % 2], w_sem.at[1]),
        )

    def results(k, which):
        out_a, out_b = outputs[2 * k : 2 * k + 2]
        if plan[k]["split"]:
            half = width // 2
            return [
                pltpu.make_async_copy(acc.at[k % 2, which, :, pl.ds(0, half)], out_a.at[which], out_sem.at[k % 2, 2 * which]),
                pltpu.make_async_copy(acc.at[k % 2, which, :, pl.ds(half, half)], out_b.at[which], out_sem.at[k % 2, 2 * which + 1]),
            ]
        return [pltpu.make_async_copy(acc.at[k % 2, which], (out_a, out_b)[which], out_sem.at[k % 2, 2 * which])]

    slot = step % 2

    @pl.when(step == 0)
    def _():
        for copy in weights(0)[1]:
            copy.start()
        fetch(0, 0)

    if turn_at is not None:
        barrier, keep, first, second, last = plane_gather(own_block, outputs[-2], *gather_sems[:3])
        far = arrays[late].at[pl.ds(pl.multiple_of(pair_rank(flipped(me, X)) * tile, tile), tile)]
        far_copy = pltpu.make_async_remote_copy(
            src_ref=far, dst_ref=far, send_sem=gather_sems[3].at[0], recv_sem=gather_sems[3].at[1], device_id=(flipped(me, CORE),), device_id_type=pl.DeviceIdType.MESH
        )

        @pl.when(step == 0)
        def _():
            barrier()
            for copy in first + [keep, far_copy]:
                copy.start()

        @pl.when(step == 2)
        def _():
            far_copy.wait_recv()

    @pl.when(fresh)
    def _():
        copies = weights(0)[1]
        copies[0].wait()
        shift = weights(0)[0]
        for k in range(1, len(plan)):
            shift = jnp.where(index == k, weights(k)[0], shift)
        chosen = lax.broadcasted_iota(jnp.int32, (block, span), 0) + shift
        chosen = (chosen == lax.broadcasted_iota(jnp.int32, (block, span), 1)).astype(jnp.bfloat16)
        w_in_t[...] = dot_nt(chosen, window[...]).astype(jnp.bfloat16)
        copies[1].wait()

    for k in range(2, len(plan)):
        @pl.when(step == begins[k])
        def _(k=k):
            for copy in results(k - 2, 0) + results(k - 2, 1):
                copy.wait()

    for k, end in enumerate(ends[:-1]):
        @pl.when(step == end - 1)
        def _(k=k):
            for copy in weights(k + 1)[1]:
                copy.start()

    @pl.when(step + 1 < steps)
    def _():
        fetch(step + 1, 1 - slot)

    pltpu.make_async_copy(arrays[0].at[pl.ds(0, tile)], hidden_buf.at[slot], sem.at[0, slot]).wait()
    pltpu.make_async_copy(arrays[0].at[pl.ds(0, tile)], grad_buf.at[slot], sem.at[1, slot]).wait()

    rows = tile // parts
    for part in range(parts):
        at = pl.ds(part * rows, rows)
        u = rounded(dot_nt(w_in_t[...], hidden_buf[slot, at]))
        e = rounded(dot_nt(w_out_buf[side], grad_buf[slot, at]))
        act, slope = gelu_parts(u)
        act_buf[:, at] = act.astype(jnp.bfloat16)
        pre_buf[:, at] = (slope * e).astype(jnp.bfloat16)

    for which, left, right in ((0, act_buf, grad_buf), (1, pre_buf, hidden_buf)):
        value = dot_nn(left[...], right[slot])

        @pl.when(fresh)
        def _():
            acc[side, which] = value

        @pl.when(jnp.logical_not(fresh))
        def _():
            acc[side, which] += value

        for k, end in enumerate(ends):
            @pl.when(step == end - 1)
            def _(k=k):
                for copy in results(k, which):
                    copy.start()

        if turn_at is not None and which == 0:
            @pl.when(step == turn_at)
            def _():
                for copy in first[:2]:
                    copy.wait_recv()
                for copy in second:
                    copy.start()

            @pl.when(step == steps - 1)
            def _():
                for copy in second[:2]:
                    copy.wait_recv()
                for copy in last:
                    copy.start()

    @pl.when(step == steps - 1)
    def _():
        if turn_at is not None:
            keep.wait()
            first[2].wait_recv()
            for copy in second[2:] + last:
                copy.wait_recv()
            for copy in first + second + last + [far_copy]:
                copy.wait_send()
        for k in range(max(0, len(plan) - 2), len(plan)):
            for copy in results(k, 0) + results(k, 1):
                copy.wait()


def column_grads(segments, w_in, w_out, gathered=None, turn_at=None, unfinished=None, collective_id=None):
    arrays, plan = [], []

    def place(array):
        for n, other in enumerate(arrays):
            if other is array:
                return n
        arrays.append(array)
        return len(arrays) - 1

    for hidden, grad, layer, bits, split in segments:
        plan.append(dict(hidden=[place(a) for a in hidden], grad=[place(a) for a in grad], layer=layer, bits=bits, split=split))
    width = arrays[0].shape[1]
    block = w_in.shape[2] // DEVICES
    span = -(-(block + 128) // 128) * 128
    tile = 1024
    tokens = sum(arrays[h].shape[0] for segment in plan for h in segment["hidden"])
    shapes = [(2, block, width // 2) if segment["split"] else (block, width) for segment in plan for _ in range(2)]
    out_shape = [jax.ShapeDtypeStruct(shape, jnp.float32) for shape in shapes]
    bf16 = jnp.bfloat16
    params, late, aliases = {}, None, {}
    if gathered is not None:
        late = place(unfinished)
        arrays.append(gathered)
        out_shape.append(jax.ShapeDtypeStruct((8,) + gathered.shape, bf16))
        out_shape.append(jax.ShapeDtypeStruct(unfinished.shape, bf16))
        aliases = {late: len(out_shape) - 1}
        params = dict(collective_id=collective_id, has_side_effects=True)
    hbm = pl.BlockSpec(memory_space=pl.ANY)
    return pl.pallas_call(
        functools.partial(grads_body, plan, len(arrays), len(out_shape), tile, 2, turn_at, late),
        grid=(tokens // tile,),
        out_shape=out_shape,
        in_specs=[hbm] * (len(arrays) + 2),
        out_specs=[hbm] * len(out_shape),
        scratch_shapes=[pltpu.VMEM((2, tile, width), bf16)] * 2
        + [pltpu.VMEM((block, tile), bf16)] * 2
        + [pltpu.VMEM((width, span), bf16), pltpu.VMEM((block, width), bf16), pltpu.VMEM((2, block, width), bf16)]
        + [pltpu.VMEM((2, 2, block, width), jnp.float32)]
        + [pltpu.SemaphoreType.DMA((2, 2)), pltpu.SemaphoreType.DMA((2,)), pltpu.SemaphoreType.DMA((2, 4))]
        + (GATHER_SEMS + [pltpu.SemaphoreType.DMA((2,))] if gathered is not None else []),
        input_output_aliases=aliases,
        compiler_params=pltpu.CompilerParams(vmem_limit_bytes=62 * 2**20, dimension_semantics=("arbitrary",), **params),
        cost_estimate=pl.CostEstimate(
            flops=8 * tokens * block * width, bytes_accessed=4 * tokens * width + 12 * block * width * len(plan), transcendentals=tokens * block
        ),
        name="column_grads",
    )(*arrays, w_in, w_out)


FF_TILE = 1280


def layers_body(scale, parts, tiles, *refs):
    tokens, targets, w_in, w_out, every, hidden_all, grad_all, below = refs[:8]
    now, target, acc, pre_buf, send_sem, recv_sem, own_sem, pair_send, pair_recv, local = refs[8:]
    step = pl.program_id(0)
    phase, tile = step // tiles, step % tiles
    me = lax.axis_index(AXIS)
    rows = now.shape[0] // parts
    _, keep, first, second, last = plane_gather(tokens, every, send_sem, recv_sem, own_sem)

    def remote(array, came, bits, n):
        place = array.at[pair_rank(flipped(me, came))]
        return pltpu.make_async_remote_copy(
            src_ref=place, dst_ref=place, send_sem=pair_send.at[n], recv_sem=pair_recv.at[n], device_id=(flipped(me, bits),), device_id_type=pl.DeviceIdType.MESH
        )

    def pair(array, n):
        store = pltpu.make_async_copy(now, array.at[pair_rank(me)], local.at[n])
        return store, remote(array, 0, X, 3 * n), remote(array, 0, CORE, 3 * n + 1)

    hidden_copies, grad_copies = pair(hidden_all, 0) + (remote(hidden_all, X, CORE, 2),), pair(grad_all, 1)
    get_tokens = pltpu.make_async_copy(tokens, now, local.at[2])
    get_target = pltpu.make_async_copy(targets, target, local.at[3])
    put_below = pltpu.make_async_copy(now, below, local.at[4])

    def on(at):
        return pl.when(step == at)

    @on(0)
    def _():
        get_tokens.start()
        get_target.start()
        ready = pltpu.get_barrier_semaphore()
        for bits in (CORE, X, Y, Z):
            pl.semaphore_signal(ready, inc=1, device_id=(flipped(me, bits),), device_id_type=pl.DeviceIdType.MESH)
        pl.semaphore_wait(ready, 4)
        for copy in first + [keep]:
            copy.start()
        get_tokens.wait()

    @on(tiles)
    def _():
        hidden_copies[0].wait()
        hidden_copies[1].start()
        hidden_copies[2].start()

    @on(tiles + 1)
    def _():
        for copy in first[:2]:
            copy.wait_recv()
        for copy in second:
            copy.start()

    @on(2 * tiles - 1)
    def _():
        for copy in second[:2]:
            copy.wait_recv()
        for copy in last:
            copy.start()
        get_target.wait()

    @on(2 * tiles)
    def _():
        grad_copies[0].wait()
        grad_copies[1].start()
        grad_copies[2].start()
        hidden_copies[1].wait_recv()
        hidden_copies[3].start()

    @pl.when(tile == 0)
    def _():
        acc[...] = now[...].astype(jnp.float32)

    @pl.when(phase < 2)
    def _():
        for part in range(parts):
            at = pl.ds(part * rows, rows)
            pre = dot_nn(now[at], w_in[0]).astype(jnp.bfloat16)
            pre_buf[tile, at] = pre
            act = gelu_parts(pre.astype(jnp.float32))[0].astype(jnp.bfloat16)
            acc[at] += dot_nn(act, w_out[0])

    @pl.when(phase == 2)
    def _():
        for part in range(parts):
            at = pl.ds(part * rows, rows)
            e = rounded(dot_nt(now[at], w_out[0]))
            slope = gelu_parts(pre_buf[tile, at].astype(jnp.float32))[1]
            acc[at] += dot_nt((slope * e).astype(jnp.bfloat16), w_in[0])

    @on(tiles - 1)
    def _():
        now[...] = acc[...].astype(jnp.bfloat16)
        hidden_copies[0].start()

    @on(2 * tiles - 1)
    def _():
        now[...] = ((rounded(acc[...]) - target[...].astype(jnp.float32)) * scale).astype(jnp.bfloat16)
        grad_copies[0].start()

    @on(3 * tiles - 1)
    def _():
        now[...] = acc[...].astype(jnp.bfloat16)
        put_below.start()
        grad_copies[1].wait_recv()
        keep.wait()
        put_below.wait()
        first[2].wait_recv()
        for copy in second[2:] + last:
            copy.wait_recv()
        for copy in hidden_copies[2:] + grad_copies[2:3]:
            copy.wait_recv()
        for copy in hidden_copies[1:] + grad_copies[1:3]:
            copy.wait_send()
        for copy in first + second + last:
            copy.wait_send()


def run_layers(tokens, targets, w_in, w_out, scale, collective_id):
    (rows, width), ff = tokens.shape, w_in.shape[2]
    tiles = ff // FF_TILE
    bf16 = jnp.bfloat16
    hbm = pl.BlockSpec(memory_space=pl.ANY)
    return pl.pallas_call(
        functools.partial(layers_body, scale, 2, tiles),
        grid=(3 * tiles,),
        out_shape=[jax.ShapeDtypeStruct((n, rows, width), bf16) for n in (8, 4, 4)] + [jax.ShapeDtypeStruct((rows, width), bf16)],
        in_specs=[
            hbm,
            hbm,
            pl.BlockSpec((1, width, FF_TILE), lambda s: (jnp.minimum(s // tiles, 1), 0, s % tiles)),
            pl.BlockSpec((1, FF_TILE, width), lambda s: (jnp.minimum(s // tiles, 1), s % tiles, 0)),
        ],
        out_specs=[hbm] * 4,
        scratch_shapes=[
            pltpu.VMEM((rows, width), bf16),
            pltpu.VMEM((rows, width), bf16),
            pltpu.VMEM((rows, width), jnp.float32),
            pltpu.VMEM((tiles, rows, FF_TILE), bf16),
        ]
        + GATHER_SEMS
        + [pltpu.SemaphoreType.DMA((6,)), pltpu.SemaphoreType.DMA((6,)), pltpu.SemaphoreType.DMA((5,))],
        compiler_params=pltpu.CompilerParams(
            vmem_limit_bytes=62 * 2**20, dimension_semantics=("arbitrary",), collective_id=collective_id, has_side_effects=True
        ),
        cost_estimate=pl.CostEstimate(flops=12 * rows * width * ff, bytes_accessed=12 * width * ff, transcendentals=3 * rows * ff),
        name="run_layers",
    )(tokens, targets, w_in, w_out)


def into_layer(body, inputs, in_specs, spec_of, grid, layer, shape, held):
    extra = [] if held is None else [held]
    return pl.pallas_call(
        functools.partial(body, len(inputs)),
        grid=grid,
        out_shape=jax.ShapeDtypeStruct(shape, jnp.float32),
        in_specs=in_specs + [pl.BlockSpec(memory_space=pl.ANY)] * len(extra),
        out_specs=spec_of(layer),
        input_output_aliases={len(inputs): 0} if extra else {},
        compiler_params=pltpu.CompilerParams(vmem_limit_bytes=62 * 2**20, dimension_semantics=("arbitrary",)),
    )(*inputs, *extra)


def sum_body(count, *refs):
    total = refs[0][...]
    for ref in refs[1:count]:
        total = total + ref[...]
    refs[-1][0] = total


def sum_into(parts, layer, layers, held):
    block, width = parts[0].shape
    rows = block // 5
    spec = pl.BlockSpec((rows, width), lambda i: (i, 0))
    return into_layer(sum_body, parts, [spec] * len(parts), lambda layer: pl.BlockSpec((1, rows, width), lambda i: (layer, i, 0)), (5,), layer, (layers, block, width), held)


def sum_halves_body(count, *refs):
    half = refs[0].shape[2]
    for side in range(2):
        mine = refs[side:count:2]
        total = mine[0][0]
        for ref in mine[1:]:
            total = total + ref[0]
        refs[-1][0, :, side * half : (side + 1) * half] = total


def sum_halves_into(pairs, layer, layers, held):
    _, block, half = pairs[0][0].shape
    rows = block // 5
    flat = [part for pair in pairs for part in pair]
    spec = pl.BlockSpec((1, rows, half), lambda i: (0, i, 0))
    return into_layer(sum_halves_body, flat, [spec] * len(flat), lambda layer: pl.BlockSpec((1, rows, 2 * half), lambda i: (layer, i, 0)), (5,), layer, (layers, block, 2 * half), held)


def turn_body(lead, *refs):
    for side in range(2):
        total = refs[side][lead]
        for ref in refs[2 + side : -1 : 2]:
            total = total + ref[lead]
        refs[-1][side] = total.T


def turn(parts):
    pairs = isinstance(parts[0], (list, tuple))
    block, half = (parts[0][0].shape if pairs else parts[0].shape)[-2:]
    half = half if pairs else half // 2
    step = 256
    blocks = half // step
    if pairs:
        specs = [pl.BlockSpec((1, block, step), lambda j: (1, 0, j))] * 2
        flat = [array for pair in parts for array in pair]
    else:
        specs = [pl.BlockSpec((block, step), lambda j: (0, j)), pl.BlockSpec((block, step), lambda j: (0, blocks + j))]
        flat = [array for array in parts for _ in range(2)]
    out = pl.pallas_call(
        functools.partial(turn_body, 0 if pairs else slice(None)),
        grid=(blocks,),
        out_shape=jax.ShapeDtypeStruct((2, half, block), jnp.float32),
        in_specs=specs * len(parts),
        out_specs=pl.BlockSpec((2, step, block), lambda j: (0, j, 0)),
        compiler_params=pltpu.CompilerParams(vmem_limit_bytes=62 * 2**20, dimension_semantics=("arbitrary",)),
    )(*flat)
    return out.reshape(DEVICES, 2 * half // DEVICES, block)


def join_body(count, blocks, *refs):
    out = refs[-1]
    block = blocks.shape[2]
    for i in range(blocks.shape[0]):
        out[0, :, i * block : (i + 1) * block] = blocks[i]


def join_into(blocks, layer, layers, held):
    count, rows, block = blocks.shape
    step = 32
    in_spec = pl.BlockSpec((count, step, block), lambda i: (0, i, 0))
    return into_layer(
        join_body, [blocks], [in_spec], lambda layer: pl.BlockSpec((1, step, count * block), lambda i: (layer, i, 0)), (rows // step,), layer, (layers, rows, count * block), held
    )


def solution(mesh):
    def local_grads(tokens, targets, w_in, w_out):
        layers = w_in.shape[0]
        scale = (tokens.shape[0] * DEVICES) ** -0.5

        all_tokens, hidden1_all, grad1_all, grad0 = run_layers(tokens, targets, w_in, w_out, scale, 1)
        all_tokens, hidden1_all, grad1_all = (array.reshape(-1, tokens.shape[1]) for array in (all_tokens, hidden1_all, grad1_all))
        hidden1_all = [hidden1_all]

        far_lo, far_hi, y_lo, y_hi, z_lo, z_hi, all_grad0, grad1_all = column_grads(
            [(hidden1_all, [grad1_all], 1, bits, True) for bits in (Y | Z, Y, Z)], w_in, w_out, grad0, 7, grad1_all, 0
        )
        grad1_all = [grad1_all]
        all_grad0 = all_grad0.reshape(all_tokens.shape)
        far_lo = swap(far_lo, Y)
        far_hi = swap(far_hi, Z)
        y_lo = swap(y_lo, Y)
        z_hi = swap(z_hi, Z)
        second0_x, first0_x = column_grads([([all_tokens], [all_grad0], 0, X, False)], w_in, w_out)
        first0_x = swap(first0_x, X)
        second0_x = swap(second0_x, X)
        y_hi = swap(y_hi + far_hi, Y)
        z_lo = swap(z_lo + far_lo, Z)
        *own1, second0, first0 = column_grads([(hidden1_all, grad1_all, 1, 0, True), ([all_tokens], [all_grad0], 0, 0, False)], w_in, w_out)

        def exchange(first):
            return lax.all_to_all(first, AXIS, split_axis=0, concat_axis=0, tiled=True)

        first0 = turn([first0, first0_x])
        first0 = exchange(first0)
        first1 = turn([own1, (y_lo, y_hi), (z_lo, z_hi)])
        first1 = exchange(first1)
        out_second = sum_halves_into([own1, (y_lo, y_hi), (z_lo, z_hi)], 1, layers, None)
        out_second = sum_into([second0, second0_x], 0, layers, out_second)
        out_first = join_into(first0, 0, layers, None)
        out_first = join_into(first1, 1, layers, out_first)
        return out_first, out_second

    tok_spec = P(AXIS, None)
    grad_spec = P(None, AXIS, None)
    return jax.shard_map(local_grads, mesh=mesh, in_specs=(tok_spec, tok_spec, P(), P()), out_specs=(grad_spec, grad_spec), check_vma=False)
```
